32 devices in a mesh: groups: 2 (over x), shard: 16 (over z, y, core).
Axes of the slice: x: 2, y: 2, z: 4, core: 2. Of those that a mesh axis runs over, the one named last changes fastest.
Arguments:
- echoes: float32 [1, 2, 4, 512, 8192], P(None, None, 'groups', 'shard'), parts along dimension 2, may hold values from -6 to 6
- waveform: float32 [2, 8192], replicated, may hold values from -6 to 6
- doppler_taper: float32 [512], replicated, may hold values from 0.3 to 1
- cfar_guard: int32 [4], P('groups'), parts along dimension 0, may hold values from 1 to 4, as said below
- cfar_train: int32 [4], P('groups'), parts along dimension 0, may hold values from 2 to 16
- noise_floor: float32 [4], P('groups'), parts along dimension 0, may hold values from 0.5 to 2
Outputs:
- cfar_ratio: float32 [1, 4, 512, 8192], P(None, 'groups', None, 'shard'), parts along dimension 1
The draws below stay inside these ranges and needn't reach their ends.
There are 2 independent parts, one for each index of `groups`. The reference program is written for one: setup_inputs(seed, part) draws one part's arguments, and reference() takes and returns one part's arrays. A program takes and returns all parts, laid end to end along the dimension named above; an argument that names none is the same for every part. Nothing has to cross between parts.
Inputs may be any that keep to these rules, and one draw needn't show every extreme that they name: In every draw some beam has cfar_guard 4 together with cfar_train 16; no beam has more of either.
All inputs are finite; a program needn't handle non-finite values.
Results may differ from the reference program's by a relative error of at most 0.000075.
Values sent between devices are 32-bit elements; how exact they have to be, the bound alone decides.
No kernel may reach another device: no remote copies, remote signals or barrier semaphores. Data moves between devices by JAX's collectives and lax.ppermute only.
A program may use at most 64 MiB of HBM per device.

```python
import math
import jax
import jax.numpy as jnp

NCPI = 1
BEAMS = 2
PULSES = 512
GATES = 8192
GUARD_MAX = 4
TRAIN_MAX = 16
HALO = 20


def cfar_windows(key):
    guard_key = jax.random.fold_in(key, 11)
    train_key = jax.random.fold_in(key, 12)
    pick_key = jax.random.fold_in(key, 13)
    guard_cells = jax.random.randint(guard_key, (BEAMS,), 1, GUARD_MAX + 1)
    train_cells = jax.random.randint(train_key, (BEAMS,), 2, TRAIN_MAX + 1)
    chosen = jax.random.randint(pick_key, (), 0, BEAMS)
    widest = jnp.arange(BEAMS) == chosen
    guard_cells = jnp.where(widest, GUARD_MAX, guard_cells)
    train_cells = jnp.where(widest, TRAIN_MAX, train_cells)
    return (guard_cells.astype(jnp.int32), train_cells.astype(jnp.int32))


def draw_cfar_guard(key, part):
    return cfar_windows(key)[0]


def draw_cfar_train(key, part):
    return cfar_windows(key)[1]


def block_scale(stream_key, dims, pieces, smallest, top_value):
    def one(axis_at, blocks):
        heights = jax.random.uniform(jax.random.fold_in(jax.random.fold_in(stream_key, 6), axis_at), (blocks,), jnp.float32, smallest / len(pieces), top_value / len(pieces))
        return jnp.repeat(jnp.exp(heights), dims[axis_at] // blocks).reshape((-1,) + (1,) * (len(dims) - axis_at - 1))

    level = one(*pieces[0])
    for cut in pieces[1:]:
        level = level * one(*cut)
    return level


def normal_values(stream_key, dims, width, reach, cuts=(), kind=jnp.bfloat16):
    level = block_scale(stream_key, dims, cuts, -0.22, 0.18) if cuts else 1.0
    result = jax.random.normal(stream_key, dims, jnp.float32) * width * level
    return jnp.minimum(jnp.maximum(result, -reach), reach).astype(kind)


def setup_inputs(seed: int = 0, part: int = 0) -> dict:
    key_list = jax.random.split(jax.random.key(seed), 7)
    part_keys = jax.random.split(jax.random.fold_in(key_list[6], part), 7)
    echoes = normal_values(part_keys[0], (NCPI, 2, BEAMS, PULSES, GATES), 1.0, 6.0, ((3, 16),), jnp.float32)
    waveform = normal_values(key_list[1], (2, GATES), 1.0, 6.0, (), jnp.float32)
    doppler_taper = jnp.clip(jnp.exp(jax.random.uniform(key_list[2], (PULSES,), jnp.float32, math.log(0.3), math.log(1.0))), 0.3, 1.0)
    cfar_guard = draw_cfar_guard(jax.random.fold_in(jax.random.fold_in(key_list[6], part), 71), part)
    cfar_train = draw_cfar_train(jax.random.fold_in(jax.random.fold_in(key_list[6], part), 71), part)
    noise_floor = jnp.clip(jnp.exp(jax.random.uniform(part_keys[5], (BEAMS,), jnp.float32, math.log(0.5), math.log(2.0))), 0.5, 2.0)
    return dict(echoes=echoes, waveform=waveform, doppler_taper=doppler_taper, cfar_guard=cfar_guard, cfar_train=cfar_train, noise_floor=noise_floor)


def reference(echoes, waveform, doppler_taper, cfar_guard, cfar_train, noise_floor):
    signal = echoes[:, 0] + 1j * echoes[:, 1]
    spectrum = jnp.fft.fft(signal, axis=-1)
    matched = waveform[0] - 1j * waveform[1]
    compressed = jnp.fft.ifft(spectrum * matched, axis=-1)
    tapered = compressed * doppler_taper[:, None]
    doppler = jnp.fft.fft(tapered, axis=2) / jnp.sqrt(jnp.float32(PULSES))
    power_map = jnp.real(doppler) ** 2 + jnp.imag(doppler) ** 2
    padded = jnp.pad(power_map, ((0, 0), (0, 0), (0, 0), (HALO, HALO)))
    offsets = jnp.arange(1, HALO + 1, dtype=jnp.int32)
    inside = (offsets[None, :] > cfar_guard[:, None]) & (offsets[None, :] <= (cfar_guard + cfar_train)[:, None])
    weights = inside.astype(jnp.float32)
    window_sum = jnp.zeros_like(power_map)
    for offset in range(1, HALO + 1):
        lower = padded[..., HALO - offset:HALO - offset + GATES]
        upper = padded[..., HALO + offset:HALO + offset + GATES]
        window_sum = window_sum + weights[:, offset - 1][None, :, None, None] * (lower + upper)
    noise_mean = window_sum / (2.0 * cfar_train.astype(jnp.float32))[None, :, None, None]
    return power_map / (noise_floor[None, :, None, None] + noise_mean)
```

```python
import math
from functools import partial

import jax
import jax.numpy as jnp
import numpy as np
from jax import lax
from jax.experimental import pallas as pl
from jax.experimental.pallas import tpu as pltpu
from jax.sharding import PartitionSpec as P


LANES = 128
SUB = 8
EDGE = 24
RADIX = 8
HALF = math.sqrt(0.5)
F32 = jnp.float32
BF16 = jnp.bfloat16


def add(x, y):
    return (x[0] + y[0], x[1] + y[1])


def sub(x, y):
    return (x[0] - y[0], x[1] - y[1])


def turn(x, sign):
    return (-x[1], x[0]) if sign > 0 else (x[1], -x[0])


def times(x, angle):
    cos, sin = math.cos(angle), math.sin(angle)
    if abs(sin) < 1e-12 and cos > 0:
        return x
    return (x[0] * cos - x[1] * sin, x[0] * sin + x[1] * cos)


def dft4(x0, x1, x2, x3, sign):
    s02, d02 = add(x0, x2), sub(x0, x2)
    s13, d13 = add(x1, x3), turn(sub(x1, x3), sign)
    return add(s02, s13), add(d02, d13), sub(s02, s13), sub(d02, d13)


def dft8(x, sign):
    even = dft4(x[0], x[2], x[4], x[6], sign)
    o0, o1, o2, o3 = dft4(x[1], x[3], x[5], x[7], sign)
    t1 = turn(o1, sign)
    t3 = turn(o3, sign)
    o1 = ((o1[0] + t1[0]) * HALF, (o1[1] + t1[1]) * HALF)
    o2 = turn(o2, sign)
    o3 = ((t3[0] - o3[0]) * HALF, (t3[1] - o3[1]) * HALF)
    odd = (o0, o1, o2, o3)
    return [add(even[i], odd[i]) for i in range(4)] + [sub(even[i], odd[i]) for i in range(4)]


def halves(x):
    high = x.astype(BF16)
    return high, (x - high.astype(F32)).astype(BF16)


def mm(left, right):
    return jnp.dot(left, right, preferred_element_type=F32)


def split_table(table):
    high = jnp.asarray(table, F32).astype(BF16)
    low = (jnp.asarray(table, F32) - high.astype(F32)).astype(BF16)
    return high, low


def dft_real(length):
    idx = np.arange(length)
    angles = 2.0 * np.pi / length * (idx[:, None] * idx[None, :] % length)
    cos, sin = np.cos(angles), np.sin(angles)
    return np.block([[cos, -sin], [sin, cos]])


def compress_body(n1, per_block, x_ref, taper_ref, tab_ref, tw1_ref, tw2_ref, filt_ref, *rest):
    outs = rest[:-2]
    stage, grid = rest[-2:]
    depth = n1 // RADIX
    taper = taper_ref[...]

    def rows(ref, i, k):
        return jnp.broadcast_to(ref[i, k : k + 1, :], (SUB, LANES))

    for b in range(depth):
        x = []
        for a in range(RADIX):
            cols = slice((depth * a + b) * LANES, (depth * a + b + 1) * LANES)
            x.append((x_ref[0, 0, 0, :, cols] * taper, x_ref[0, 1, 0, :, cols] * taper))
        for c, y in enumerate(dft8(x, -1)):
            y = times(y, -2.0 * math.pi * b * c / n1)
            stage[0, c * depth + b] = y[0]
            stage[1, c * depth + b] = y[1]
    for c in range(RADIX):
        x = [(stage[0, c * depth + b], stage[1, c * depth + b]) for b in range(depth)]
        for d, y in enumerate(dft8(x, -1)):
            k = c + RADIX * d
            cos, sin = rows(tw1_ref, 0, k), rows(tw1_ref, 1, k)
            grid[k, :, :LANES] = y[0] * cos + y[1] * sin
            grid[k, :, LANES:] = y[1] * cos - y[0] * sin
    high_tab, low_tab = tab_ref[0], tab_ref[1]

    def transform(values):
        high, low = halves(values)
        return mm(high, high_tab) + mm(low, high_tab) + mm(high, low_tab)

    spec = transform(grid[...].reshape(n1 * SUB, 2 * LANES)).reshape(n1, SUB, 2 * LANES)
    s_re, s_im = spec[:, :, :LANES], spec[:, :, LANES:]
    f_re, f_im = filt_ref[0][:, None, :], filt_ref[1][:, None, :]
    z_re = s_re * f_re + s_im * f_im
    z_im = s_re * f_im - s_im * f_re
    z = jnp.concatenate([z_re, z_im], axis=-1).reshape(n1 * SUB, 2 * LANES)
    grid[...] = transform(z).reshape(n1, SUB, 2 * LANES)
    for c in range(RADIX):
        x = []
        for d in range(depth):
            k = c + RADIX * d
            cos, sin = rows(tw2_ref, 0, k), rows(tw2_ref, 1, k)
            v_re, v_im = grid[k, :, :LANES], grid[k, :, LANES:]
            x.append((v_re * cos + v_im * sin, v_re * sin - v_im * cos))
        for b, y in enumerate(dft8(x, 1)):
            y = times(y, 2.0 * math.pi * b * c / n1)
            stage[0, b * RADIX + c] = y[0]
            stage[1, b * RADIX + c] = y[1]
    for b in range(depth):
        x = [(stage[0, b * RADIX + c], stage[1, b * RADIX + c]) for c in range(RADIX)]
        for a, y in enumerate(dft8(x, 1)):
            k, j = divmod(depth * a + b, per_block)
            outs[k][0, :, j * LANES : (j + 1) * LANES] = y[0]
            outs[k][1, :, j * LANES : (j + 1) * LANES] = y[1]


def compress(echoes, beam, taper, tab, tw1, tw2, filt, count):
    pulses, gates = echoes.shape[3:]
    n1 = gates // LANES
    width = gates // count
    full = lambda shape: pl.BlockSpec(shape, lambda i: (0,) * len(shape))
    return pl.pallas_call(
        partial(compress_body, n1, width // LANES),
        grid=(pulses // SUB,),
        in_specs=[
            pl.BlockSpec((1, 2, 1, SUB, gates), lambda i: (0, 0, beam, i, 0)),
            pl.BlockSpec((SUB, LANES), lambda i: (i, 0)),
            full(tab.shape),
            full(tw1.shape),
            full(tw2.shape),
            full(filt.shape),
        ],
        out_specs=[pl.BlockSpec((2, SUB, width), lambda i: (0, i, 0))] * count,
        out_shape=[jax.ShapeDtypeStruct((2, pulses, width), F32)] * count,
        scratch_shapes=[
            pltpu.VMEM((2, n1, SUB, LANES), F32),
            pltpu.VMEM((n1, SUB, 2 * LANES), F32),
        ],
        cost_estimate=pl.CostEstimate(
            flops=pulses * gates * 1500, transcendentals=0, bytes_accessed=pulses * gates * 16
        ),
        name="compress",
    )(echoes, taper, tab, tw1, tw2, filt)


def doppler_body(count, pulses, tab_ref, tw_ref, *rest):
    ins = rest[:count]
    power_ref, left_ref, right_ref, high_buf, low_buf = rest[count:]
    own = ins[0].shape[1]
    tiles = power_ref.shape[0]
    quarter = pulses // 4
    high_tab, low_tab = tab_ref[0], tab_ref[1]

    def load(part, start, lanes):
        slot, row = divmod(start, own)
        return ins[slot][part, row : row + SUB, lanes]

    for j in range(tiles):
        lanes = slice(j * LANES, (j + 1) * LANES)
        for r in range(0, quarter, 2 * SUB):
            x = []
            for h in range(4):
                x.append(
                    tuple(
                        jnp.concatenate(
                            [load(part, h * quarter + r + s, lanes) for s in (0, SUB)], axis=0
                        )
                        for part in range(2)
                    )
                )
            for k, y in enumerate(dft4(*x, -1)):
                if k:
                    cos = tw_ref[k - 1, 0, r : r + 2 * SUB, :]
                    sin = tw_ref[k - 1, 1, r : r + 2 * SUB, :]
                    y = (y[0] * cos + y[1] * sin, y[1] * cos - y[0] * sin)
                for part in range(2):
                    high, low = halves(y[part])
                    at = part * quarter + r
                    cols = slice(j * LANES, (j + 1) * LANES)
                    high_buf[k, at : at + 2 * SUB, cols] = high
                    low_buf[k, at : at + 2 * SUB, cols] = low
    for k in range(4):
        high, low = high_buf[k], low_buf[k]
        out = mm(high_tab, high) + mm(high_tab, low) + mm(low_tab, high)
        power = out[:quarter] * out[:quarter] + out[quarter:] * out[quarter:]
        for j in range(tiles):
            power_ref[j, pl.ds(k, quarter, stride=4), :] = power[:, j * LANES : (j + 1) * LANES]
    left_ref[...] = power_ref[0].T[:EDGE]
    right_ref[...] = power_ref[tiles - 1].T[LANES - EDGE :]


def doppler(blocks, tab, tw, pulses):
    count = len(blocks)
    width = blocks[0].shape[-1]
    tiles = width // LANES
    half = pulses // 2
    return pl.pallas_call(
        partial(doppler_body, count, pulses),
        out_shape=[
            jax.ShapeDtypeStruct((tiles, pulses, LANES), F32),
            jax.ShapeDtypeStruct((EDGE, pulses), F32),
            jax.ShapeDtypeStruct((EDGE, pulses), F32),
        ],
        scratch_shapes=[pltpu.VMEM((4, half, width), BF16), pltpu.VMEM((4, half, width), BF16)],
        cost_estimate=pl.CostEstimate(
            flops=pulses * width * 6000, transcendentals=0, bytes_accessed=pulses * width * 12
        ),
        name="doppler",
    )(tab, tw, *blocks)


def cfar_body(beam, group, win_ref, rate_ref, left_ref, right_ref, power_ref, *rest):
    out_ref, high_buf, low_buf = rest[-3:]
    tiles, pulses = power_ref.shape[:2]
    guard, train = win_ref[0, beam], win_ref[1, beam]
    floor, scale = rate_ref[0, beam], rate_ref[1, beam]
    rows = (group + 2) * LANES
    shape = (rows, group * LANES)
    away = jnp.abs(
        lax.broadcasted_iota(jnp.int32, shape, 0)
        - LANES
        - lax.broadcasted_iota(jnp.int32, shape, 1)
    )
    band = jnp.where((away > guard) & (away <= guard + train), 1.0, 0.0).astype(BF16)
    blank = jnp.zeros((LANES - EDGE, pulses), F32)
    ends = {
        0: jnp.concatenate([blank, left_ref[...]], axis=0).T,
        tiles + 1: jnp.concatenate([right_ref[...], blank], axis=0).T,
    }
    for t in range(tiles + 2):
        high, low = halves(ends[t] if t in ends else power_ref[t - 1])
        high_buf[:, t * LANES : (t + 1) * LANES] = high
        low_buf[:, t * LANES : (t + 1) * LANES] = low
    for t in range(0, tiles, group):
        cols = slice(t * LANES, t * LANES + rows)
        window = mm(high_buf[:, cols], band) + mm(low_buf[:, cols], band)
        for g in range(group):
            noise = floor + window[:, g * LANES : (g + 1) * LANES] * scale
            at = slice((t + g) * LANES, (t + g + 1) * LANES)
            out_ref[0, 0, :, at] = power_ref[t + g] / noise


def cfar(beam, beams, win, rate, left, right, power, prior):
    tiles, pulses, _ = power.shape
    width = tiles * LANES
    group = 2 if tiles % 2 == 0 else 1
    smem = pl.BlockSpec(memory_space=pltpu.SMEM)
    full = lambda shape: pl.BlockSpec(shape, lambda i: (0,) * len(shape))
    args = [win, rate, left, right, power]
    specs = [smem, smem] + [full(a.shape) for a in args[2:]]
    alias = {}
    if prior is not None:
        args.append(prior)
        specs.append(pl.BlockSpec(memory_space=pl.ANY))
        alias = {len(args) - 1: 0}
    return pl.pallas_call(
        partial(cfar_body, beam, group),
        grid=(1,),
        in_specs=specs,
        out_specs=pl.BlockSpec((1, 1, pulses, width), lambda i: (0, beam, 0, 0)),
        out_shape=jax.ShapeDtypeStruct((1, beams, pulses, width), F32),
        scratch_shapes=[pltpu.VMEM((pulses, width + 2 * LANES), BF16)] * 2,
        input_output_aliases=alias,
        cost_estimate=pl.CostEstimate(
            flops=pulses * width * 4000, transcendentals=0, bytes_accessed=pulses * width * 8
        ),
        name="cfar",
    )(*args)


def exchange(blocks, axis, count):
    if count > 16:
        me = lax.axis_index(axis)
        got = lax.all_to_all(jnp.roll(jnp.stack(blocks), me, 0), axis, 0, 0, tiled=True)
        got = jnp.roll(got, -me, 0)
        return [got[i] for i in range(count)]
    got = [blocks[0]] + [None] * (count - 1)
    for k in range(1, count):
        ring = [(i, (i + k) % count) for i in range(count)]
        got[(count - k) % count] = lax.ppermute(blocks[k], axis, ring)
    return got


def shards(axis, echoes, waveform, doppler_taper, cfar_guard, cfar_train, noise_floor):
    count = lax.axis_size(axis)
    me = lax.axis_index(axis)
    beams, own, gates = echoes.shape[2:]
    pulses = own * count
    n1 = gates // LANES
    width = gates // count

    tab = jnp.stack(split_table(dft_real(LANES)))
    k1 = jnp.arange(n1, dtype=jnp.int32)[:, None]
    n2 = jnp.arange(LANES, dtype=jnp.int32)[None, :]
    step = 2.0 * math.pi / gates
    fwd = step * (k1 * n2 % gates).astype(F32)
    back = step * (k1 * (n2 + me * width) % gates).astype(F32)
    tw1 = jnp.stack([jnp.cos(fwd), jnp.sin(fwd)])
    tw2 = jnp.stack([jnp.cos(back), jnp.sin(back)]) * (1.0 / gates)
    filt = waveform.reshape(2, LANES, n1).swapaxes(1, 2)
    taper = lax.dynamic_slice(doppler_taper, (me * own,), (own,)) * (1.0 / math.sqrt(pulses))
    taper = jnp.broadcast_to(taper[:, None], (own, LANES))

    quarter = pulses // 4
    dop_tab = jnp.stack(split_table(dft_real(quarter).T))
    turns = 2.0 * np.pi / pulses * (np.arange(1, 4)[:, None] * np.arange(quarter)[None, :])
    turns = np.stack([np.cos(turns), np.sin(turns)], axis=1)
    dop_tw = jnp.broadcast_to(jnp.asarray(turns, F32)[..., None], turns.shape + (LANES,))
    win = jnp.stack([cfar_guard, cfar_train])
    rate = jnp.stack([noise_floor, 0.5 / cfar_train.astype(F32)])

    sent = []
    for beam in range(beams):
        blocks = compress(echoes, beam, taper, tab, tw1, tw2, filt, count)
        sent.append(exchange(blocks, axis, count))
    result = None
    for beam in range(beams):
        power, first, last = doppler(sent[beam], dop_tab, dop_tw, pulses)
        left = lax.ppermute(last, axis, [(i, i + 1) for i in range(count - 1)])
        right = lax.ppermute(first, axis, [(i + 1, i) for i in range(count - 1)])
        result = cfar(beam, beams, win, rate, left, right, power, result)
    return result


def solution(mesh):
    in_specs = (
        P(None, None, "groups", "shard", None),
        P(),
        P(),
        P("groups"),
        P("groups"),
        P("groups"),
    )
    out_specs = P(None, "groups", None, "shard")
    return jax.shard_map(
        partial(shards, "shard"), mesh=mesh, in_specs=in_specs, out_specs=out_specs, check_vma=False
    )
```

```python
import math
from functools import partial

import jax
import jax.numpy as jnp
import numpy as np
from jax import lax
from jax.experimental import pallas as pl
from jax.experimental.pallas import tpu as pltpu
from jax.sharding import PartitionSpec as P


LANES = 128
SUB = 8
EDGE = 24
RADIX = 8
GROUPS = 1
MODES = (True, True, False)
HALF = math.sqrt(0.5)
F32 = jnp.float32
BF16 = jnp.bfloat16


def add(x, y):
    return (x[0] + y[0], x[1] + y[1])


def sub(x, y):
    return (x[0] - y[0], x[1] - y[1])


def turn(x, sign):
    return (-x[1], x[0]) if sign > 0 else (x[1], -x[0])


def times(x, angle):
    cos, sin = math.cos(angle), math.sin(angle)
    if abs(sin) < 1e-12 and cos > 0:
        return x
    return (x[0] * cos - x[1] * sin, x[0] * sin + x[1] * cos)


def dft4(x0, x1, x2, x3, sign):
    s02, d02 = add(x0, x2), sub(x0, x2)
    s13, d13 = add(x1, x3), turn(sub(x1, x3), sign)
    return add(s02, s13), add(d02, d13), sub(s02, s13), sub(d02, d13)


def dft8(x, sign):
    even = dft4(x[0], x[2], x[4], x[6], sign)
    o0, o1, o2, o3 = dft4(x[1], x[3], x[5], x[7], sign)
    t1 = turn(o1, sign)
    t3 = turn(o3, sign)
    o1 = ((o1[0] + t1[0]) * HALF, (o1[1] + t1[1]) * HALF)
    o2 = turn(o2, sign)
    o3 = ((t3[0] - o3[0]) * HALF, (t3[1] - o3[1]) * HALF)
    odd = (o0, o1, o2, o3)
    return [add(even[i], odd[i]) for i in range(4)] + [sub(even[i], odd[i]) for i in range(4)]


def halves(x):
    high = x.astype(BF16)
    return high, (x - high.astype(F32)).astype(BF16)


def mm(left, right):
    return jnp.dot(left, right, preferred_element_type=F32)


def split_table(table):
    table = np.asarray(table, np.float32)
    high = table.astype(BF16)
    low = (table - high.astype(np.float32)).astype(BF16)
    return jnp.asarray(np.stack([high, low]))


def dft_real(length):
    idx = np.arange(length)
    angles = 2.0 * np.pi / length * (idx[:, None] * idx[None, :] % length)
    cos, sin = np.cos(angles), np.sin(angles)
    return np.block([[cos, -sin], [sin, cos]])


def three(high, low):
    return jnp.concatenate([high, low, high], axis=-1)


def prepare(axis, n1, wave_ref, tw1_ref, phase_ref, tw2_ref, filt_ref, flat):
    me = lax.axis_index(axis)
    count = phase_ref.shape[1]
    ways = LANES // n1
    for part in range(2):
        for m in range(n1):
            flat[m : m + 1, :] = wave_ref[part : part + 1, m * LANES : (m + 1) * LANES]
        rows = flat[:n1, :]
        for h in range(ways):
            moved = pltpu.roll(rows, LANES - h * n1, 1) if h else rows
            flat[pl.ds(h, n1, stride=ways), :] = moved
        filt_ref[part] = flat[...].T[:n1]
    for part in range(2):
        for k in range(n1):
            at = k * me % count
            tw2_ref[part, k : k + 1, :] = phase_ref[part, pl.ds(at, 1), :]
    turn_re, turn_im = tw2_ref[0], tw2_ref[1]
    cos, sin = tw1_ref[0], tw1_ref[1]
    tw2_ref[0] = cos * turn_re - sin * turn_im
    tw2_ref[1] = sin * turn_re + cos * turn_im


def compress_body(axis, pieces, hops, count, x_ref, taper_ref, wave_ref, tab_ref, tw1_ref, phase_ref, *rest):
    me = lax.axis_index(axis)
    outs, used = [], 0
    for hop in hops:
        if hop:
            outs.append(rest[used : used + count])
            used += count
        else:
            outs.append([rest[used].at[(me + k) % count] for k in range(count)])
            used += 1
    stage, grid, tw2_ref, filt_ref, flat = rest[used:]
    own = x_ref.shape[3]
    n1 = x_ref.shape[4] // LANES
    depth = n1 // RADIX
    tiles = n1 // count
    step = pl.program_id(0)

    @pl.when(step == 0)
    def _():
        prepare(axis, n1, wave_ref, tw1_ref, phase_ref, tw2_ref, filt_ref, flat)

    def rows(ref, i, k):
        return jnp.broadcast_to(ref[i, k : k + 1, :], (SUB, LANES))

    place = {}
    for p, piece in enumerate(pieces):
        for at, tile in enumerate(piece):
            place[tile] = (p, at)
    row = lax.broadcasted_iota(jnp.int32, (SUB, LANES), 0)
    first = (me * pl.num_programs(0) + step) * own
    root = 1.0 / math.sqrt(taper_ref.shape[0])
    for g in range(own // SUB):
        at = slice(g * SUB, (g + 1) * SUB)
        taper = jnp.full((SUB, LANES), taper_ref[first + g * SUB])
        for r in range(1, SUB):
            taper = jnp.where(row == r, taper_ref[first + g * SUB + r], taper)
        taper = taper * root
        for b in range(depth):
            x = []
            for a in range(RADIX):
                cols = slice((depth * a + b) * LANES, (depth * a + b + 1) * LANES)
                x.append((x_ref[0, 0, 0, at, cols] * taper, x_ref[0, 1, 0, at, cols] * taper))
            for c, y in enumerate(dft8(x, -1)):
                y = times(y, -2.0 * math.pi * b * c / n1)
                stage[0, c * depth + b] = y[0]
                stage[1, c * depth + b] = y[1]
        for c in range(RADIX):
            x = [(stage[0, c * depth + b], stage[1, c * depth + b]) for b in range(depth)]
            for d, y in enumerate(dft8(x, -1)):
                k = c + RADIX * d
                cos, sin = rows(tw1_ref, 0, k), rows(tw1_ref, 1, k)
                grid[k, at, :LANES] = y[0] * cos + y[1] * sin
                grid[k, at, LANES:] = y[1] * cos - y[0] * sin
    table = jnp.concatenate([tab_ref[0], tab_ref[0], tab_ref[1]], axis=0)
    flat_rows = n1 * own
    spec = mm(three(*halves(grid[...].reshape(flat_rows, 2 * LANES))), table)
    spec = spec.reshape(n1, own, 2 * LANES)
    s_re, s_im = spec[:, :, :LANES], spec[:, :, LANES:]
    f_re, f_im = filt_ref[0][:, None, :], filt_ref[1][:, None, :]
    z_re = s_re * f_re + s_im * f_im
    z_im = s_re * f_im - s_im * f_re
    z = jnp.concatenate([z_re, z_im], axis=-1).reshape(flat_rows, 2 * LANES)
    grid[...] = mm(three(*halves(z)), table).reshape(n1, own, 2 * LANES)
    for g in range(own // SUB):
        at = slice(g * SUB, (g + 1) * SUB)
        for c in range(RADIX):
            x = []
            for d in range(depth):
                k = c + RADIX * d
                cos, sin = rows(tw2_ref, 0, k), rows(tw2_ref, 1, k)
                v_re, v_im = grid[k, at, :LANES], grid[k, at, LANES:]
                x.append((v_re * cos + v_im * sin, v_re * sin - v_im * cos))
            for b, y in enumerate(dft8(x, 1)):
                y = times(y, 2.0 * math.pi * b * c / n1)
                stage[0, b * RADIX + c] = y[0]
                stage[1, b * RADIX + c] = y[1]
        for b in range(depth):
            x = [(stage[0, b * RADIX + c], stage[1, b * RADIX + c]) for c in range(RADIX)]
            for a, y in enumerate(dft8(x, 1)):
                k, j = divmod(depth * a + b, tiles)
                p, to = place[j]
                out = outs[p][k]
                out[0, at, to * LANES : (to + 1) * LANES] = y[0]
                out[1, at, to * LANES : (to + 1) * LANES] = y[1]


def whole(shape):
    return pl.BlockSpec(shape, lambda i: (0,) * len(shape))


def compress(axis, echoes, beam, pieces, hops, taper, wave, tab, tw1, phase):
    pulses, gates = echoes.shape[3:]
    count = phase.shape[1]
    n1 = gates // LANES
    size = math.gcd(pulses, SUB * GROUPS)
    shapes, specs = [], []
    for piece, hop in zip(pieces, hops):
        wide = len(piece) * LANES
        if hop:
            shapes += [jax.ShapeDtypeStruct((2, pulses, wide), F32)] * count
            specs += [pl.BlockSpec((2, size, wide), lambda i: (0, i, 0))] * count
        else:
            shapes.append(jax.ShapeDtypeStruct((count, 2, pulses, wide), F32))
            specs.append(pl.BlockSpec((count, 2, size, wide), lambda i: (0, 0, i, 0)))
    out = pl.pallas_call(
        partial(compress_body, axis, pieces, hops, count),
        grid=(pulses // size,),
        in_specs=[
            pl.BlockSpec((1, 2, 1, size, gates), lambda i: (0, 0, beam, i, 0)),
            pl.BlockSpec(memory_space=pltpu.SMEM),
            whole(wave.shape),
            whole(tab.shape),
            whole(tw1.shape),
            whole(phase.shape),
        ],
        out_specs=specs,
        out_shape=shapes,
        scratch_shapes=[
            pltpu.VMEM((2, n1, SUB, LANES), F32),
            pltpu.VMEM((n1, size, 2 * LANES), F32),
            pltpu.VMEM((2, n1, LANES), F32),
            pltpu.VMEM((2, n1, LANES), F32),
            pltpu.VMEM((LANES, LANES), F32),
        ],
        cost_estimate=pl.CostEstimate(
            flops=pulses * gates * 6000, transcendentals=0, bytes_accessed=pulses * gates * 16
        ),
        name="compress",
    )(echoes, taper, wave, tab, tw1, phase)
    blocks = []
    for hop in hops:
        blocks.append(out[:count] if hop else out[0])
        out = out[count if hop else 1 :]
    return blocks


def doppler_core(ins, pulses, tab_ref, tw_ref, high_buf, low_buf, emit):
    if len(ins) == 1:
        ins = [ins[0].at[k] for k in range(ins[0].shape[0])]
    own = ins[0].shape[1]
    tiles = ins[0].shape[2] // LANES
    quarter = pulses // 4

    def load(part, start, lanes):
        slot, row = divmod(start, own)
        return ins[slot][part, row : row + SUB, lanes]

    for r in range(0, quarter, 2 * SUB):
        for j in range(tiles):
            lanes = slice(j * LANES, (j + 1) * LANES)
            x = []
            for h in range(4):
                x.append(
                    tuple(
                        jnp.concatenate(
                            [load(part, h * quarter + r + s, lanes) for s in (0, SUB)], axis=0
                        )
                        for part in range(2)
                    )
                )
            for k, y in enumerate(dft4(*x, -1)):
                if k:
                    cos = tw_ref[k - 1, 0, r : r + 2 * SUB, :]
                    sin = tw_ref[k - 1, 1, r : r + 2 * SUB, :]
                    y = (y[0] * cos + y[1] * sin, y[1] * cos - y[0] * sin)
                for part in range(2):
                    high, low = halves(y[part])
                    at = part * quarter + r
                    high_buf[k, at : at + 2 * SUB, lanes] = high
                    low_buf[k, at : at + 2 * SUB, lanes] = low
    table = jnp.concatenate([tab_ref[0], tab_ref[0], tab_ref[1]], axis=1)
    for k in range(4):
        high, low = high_buf[k], low_buf[k]
        out = mm(table, jnp.concatenate([high, low, high], axis=0))
        power = out[:quarter] * out[:quarter] + out[quarter:] * out[quarter:]
        for j in range(tiles):
            emit(j, pl.ds(k, quarter, stride=4), power[:, j * LANES : (j + 1) * LANES])


def doppler_body(count, pulses, ends, tab_ref, tw_ref, *rest):
    ins = rest[:count]
    power_ref, left_ref, right_ref, high_buf, low_buf = rest[count:]

    def emit(j, rows, value):
        power_ref[j, rows, :] = value

    doppler_core(ins, pulses, tab_ref, tw_ref, high_buf, low_buf, emit)
    left_ref[...] = power_ref[ends[0]].T[:EDGE]
    right_ref[...] = power_ref[ends[1]].T[LANES - EDGE :]


def doppler(blocks, tab, tw, pulses, ends):
    count = len(blocks)
    width = blocks[0].shape[-1]
    tiles = width // LANES
    half = pulses // 2
    return pl.pallas_call(
        partial(doppler_body, count, pulses, ends),
        out_shape=[
            jax.ShapeDtypeStruct((tiles, pulses, LANES), F32),
            jax.ShapeDtypeStruct((EDGE, pulses), F32),
            jax.ShapeDtypeStruct((EDGE, pulses), F32),
        ],
        scratch_shapes=[pltpu.VMEM((4, half, width), BF16), pltpu.VMEM((4, half, width), BF16)],
        cost_estimate=pl.CostEstimate(
            flops=pulses * width * 6000, transcendentals=0, bytes_accessed=pulses * width * 12
        ),
        name="doppler",
    )(tab, tw, *blocks)


def cfar_core(beam, tiles, guard_ref, train_ref, floor_ref, left, right, tile, high_buf, low_buf, emit):
    pulses = high_buf.shape[0]
    group = 2 if tiles % 2 == 0 else 1
    guard, train = guard_ref[beam], train_ref[beam]
    width = group * LANES
    rows = width + 2 * LANES
    shape = (rows, width)
    away = jnp.abs(
        lax.broadcasted_iota(jnp.int32, shape, 0)
        - LANES
        - lax.broadcasted_iota(jnp.int32, shape, 1)
    )
    band = jnp.where((away > guard) & (away <= guard + train), 1.0, 0.0).astype(BF16)
    blank = jnp.zeros((LANES - EDGE, pulses), F32)
    floor = jnp.full((1, LANES), floor_ref[beam])
    scale = 0.5 / jnp.full((1, LANES), train.astype(F32))
    for t in range(tiles + 2):
        if t == 0:
            values = jnp.concatenate([blank, left], axis=0).T
        elif t == tiles + 1:
            values = jnp.concatenate([right, blank], axis=0).T
        else:
            values = tile(t - 1)
        high, low = halves(values)
        high_buf[:, t * LANES : (t + 1) * LANES] = high
        low_buf[:, t * LANES : (t + 1) * LANES] = low
    twice = jnp.concatenate([band, band], axis=0)
    for t in range(0, tiles, group):
        cols = slice(t * LANES, t * LANES + rows)
        window = mm(jnp.concatenate([high_buf[:, cols], low_buf[:, cols]], axis=1), twice)
        for g in range(group):
            noise = floor + window[:, g * LANES : (g + 1) * LANES] * scale
            emit(t + g, tile(t + g) / noise)


def finish_body(beam, count, known, fresh, pulses, *refs):
    guard_ref, train_ref, floor_ref, left_ref, right_ref = refs[:5]
    refs = refs[5:]
    tiles = len(known) + len(fresh)
    old = new = None
    if known:
        old, refs = refs[0], refs[1:]
    if fresh:
        tab_ref, tw_ref = refs[:2]
        ins = refs[2 : 2 + count]
        refs = refs[2 + count :]
    bufs = refs[len(refs) - (5 if fresh else 2) :]
    out_ref = refs[len(refs) - len(bufs) - 1]
    if fresh:
        new = bufs[4]

        def keep(j, rows, value):
            new[j, rows, :] = value

        doppler_core(ins, pulses, tab_ref, tw_ref, bufs[2], bufs[3], keep)

    def tile(t):
        return old[known.index(t)] if t in known else new[fresh.index(t)]

    def emit(t, value):
        out_ref[0, 0, :, t * LANES : (t + 1) * LANES] = value

    cfar_core(
        beam, tiles, guard_ref, train_ref, floor_ref, left_ref[...], right_ref[...], tile, bufs[0], bufs[1], emit
    )


def finish(beam, beams, scalars, left, right, known, power, fresh, blocks, tables, prior):
    pulses = left.shape[1]
    tiles = len(known) + len(fresh)
    width = tiles * LANES
    smem = pl.BlockSpec(memory_space=pltpu.SMEM)
    args = list(scalars) + [left, right]
    if known:
        args.append(power)
    if fresh:
        args += list(tables) + list(blocks)
    specs = [smem] * len(scalars) + [whole(a.shape) for a in args[len(scalars) :]]
    alias = {}
    if prior is not None:
        args.append(prior)
        specs.append(pl.BlockSpec(memory_space=pl.ANY))
        alias = {len(args) - 1: 0}
    scratch = [pltpu.VMEM((pulses, width + 2 * LANES), BF16)] * 2
    if fresh:
        scratch += [pltpu.VMEM((4, pulses // 2, len(fresh) * LANES), BF16)] * 2
        scratch += [pltpu.VMEM((len(fresh), pulses, LANES), F32)]
    return pl.pallas_call(
        partial(finish_body, beam, len(blocks), known, fresh, pulses),
        grid=(1,),
        in_specs=specs,
        out_specs=pl.BlockSpec((1, 1, pulses, width), lambda i: (0, beam, 0, 0)),
        out_shape=jax.ShapeDtypeStruct((1, beams, pulses, width), F32),
        scratch_shapes=scratch,
        input_output_aliases=alias,
        cost_estimate=pl.CostEstimate(
            flops=pulses * width * 4000, transcendentals=0, bytes_accessed=pulses * width * 8
        ),
        name="finish",
    )(*args)


def exchange(blocks, axis):
    if not isinstance(blocks, (tuple, list)):
        return [lax.all_to_all(blocks, axis, 0, 0, tiled=True)]
    count = len(blocks)
    got = [blocks[0]] + [None] * (count - 1)
    for k in range(1, count):
        ring = [(i, (i + k) % count) for i in range(count)]
        got[(count - k) % count] = lax.ppermute(blocks[k], axis, ring)
    return got


def modes(count):
    return MODES if count <= 16 else (False,) * len(MODES)


def halo(axis, first, last):
    count = lax.axis_size(axis)
    left = lax.ppermute(last, axis, [(i, i + 1) for i in range(count - 1)])
    right = lax.ppermute(first, axis, [(i + 1, i) for i in range(count - 1)])
    return left, right


def shards_inner(axis, echoes, waveform, doppler_taper, cfar_guard, cfar_train, noise_floor):
    count = lax.axis_size(axis)
    beams, own, gates = echoes.shape[2:]
    pulses = own * count
    n1 = gates // LANES
    tiles = n1 // count

    tab = split_table(dft_real(LANES))
    angles = 2.0 * np.pi / gates * (np.arange(n1)[:, None] * np.arange(LANES)[None, :])
    tw1 = jnp.asarray(np.stack([np.cos(angles), np.sin(angles)]), F32)
    angles = 2.0 * np.pi / count * np.arange(count)
    phase = np.stack([np.cos(angles), np.sin(angles)])[..., None] / gates
    phase = jnp.asarray(np.broadcast_to(phase, phase.shape[:2] + (LANES,)), F32)
    quarter = pulses // 4
    dop_tab = split_table(dft_real(quarter).T)
    turns = 2.0 * np.pi / pulses * (np.arange(1, 4)[:, None] * np.arange(quarter)[None, :])
    turns = np.stack([np.cos(turns), np.sin(turns)], axis=1)[..., None]
    dop_tw = jnp.asarray(np.broadcast_to(turns, turns.shape[:3] + (LANES,)), F32)
    tables = (dop_tab, dop_tw)
    scalars = (cfar_guard, cfar_train, noise_floor)

    every = tuple(range(tiles))
    middle = every[tiles // 2 : tiles // 2 + 1] if tiles > 2 else ()
    outer = tuple(t for t in every if t not in middle)
    built = []
    for beam in range(beams):
        split = middle and beam == beams - 1
        pieces = (outer, middle) if split else (every,)
        hops = modes(count)[len(built) : len(built) + len(pieces)]
        blocks = compress(
            axis, echoes, beam, pieces, hops, doppler_taper, waveform, tab, tw1, phase
        )
        built += [(beam, piece, block) for piece, block in zip(pieces, blocks)]
    sent = []
    for beam, piece, block in built:
        sent.append((beam, piece, exchange(block, axis)))
    known = []
    late = None
    gate = [block[0] if isinstance(block, list) else block for _, _, block in built]
    for beam, piece, blocks in sent:
        if 0 not in piece:
            late = (piece, blocks)
            continue
        blocks, gate = lax.optimization_barrier((blocks, gate))
        power, first, last = doppler(blocks, *tables, pulses, (0, len(piece) - 1))
        gate = (gate, power)
        left, right = halo(axis, first, last)
        known.append((beam, left, right, piece, power))
    result = None
    for beam, left, right, piece, power in known:
        args = (beam, beams, scalars, left, right, piece, power)
        if len(piece) < tiles:
            fresh, blocks = late
            blocks, result = lax.optimization_barrier((blocks, result))
            result = finish(*args, fresh, blocks, tables, result)
        else:
            result = finish(*args, (), (), tables, result)
    return result


def shards(axis, *args):
    return shards_inner(axis, *args)


def solution(mesh):
    in_specs = (
        P(None, None, "groups", "shard", None),
        P(),
        P(),
        P("groups"),
        P("groups"),
        P("groups"),
    )
    out_specs = P(None, "groups", None, "shard")
    return jax.shard_map(
        partial(shards, "shard"), mesh=mesh, in_specs=in_specs, out_specs=out_specs, check_vma=False
    )
```

```python
import math
from functools import partial

import jax
import jax.numpy as jnp
import numpy as np
from jax import lax
from jax.experimental import pallas as pl
from jax.experimental.pallas import tpu as pltpu
from jax.sharding import PartitionSpec as P


LANES = 128
SUB = 8
EDGE = 24
RADIX = 8
GROUPS = 2
CHUNKS = 8
MODES = (True, True, False)
HALF = math.sqrt(0.5)
F32 = jnp.float32
BF16 = jnp.bfloat16


def add(x, y):
    return (x[0] + y[0], x[1] + y[1])


def sub(x, y):
    return (x[0] - y[0], x[1] - y[1])


def plus_turn(x, y, sign):
    return (x[0] - y[1], x[1] + y[0]) if sign > 0 else (x[0] + y[1], x[1] - y[0])


def times(x, angle):
    cos, sin = math.cos(angle), math.sin(angle)
    if abs(sin) < 1e-12 and cos > 0:
        return x
    return (x[0] * cos - x[1] * sin, x[0] * sin + x[1] * cos)


def dft4(x0, x1, x2, x3, sign):
    s02, d02 = add(x0, x2), sub(x0, x2)
    s13, d13 = add(x1, x3), sub(x1, x3)
    first, third = plus_turn(d02, d13, sign), plus_turn(d02, d13, -sign)
    return add(s02, s13), first, sub(s02, s13), third


def dft8(x, sign):
    e0, e1, e2, e3 = dft4(x[0], x[2], x[4], x[6], sign)
    o0, o1, o2, o3 = dft4(x[1], x[3], x[5], x[7], sign)
    o1 = tuple(v * HALF for v in plus_turn(o1, o1, sign))
    o3 = tuple(v * HALF for v in plus_turn(o3, o3, -sign))
    return [
        add(e0, o0),
        add(e1, o1),
        plus_turn(e2, o2, sign),
        sub(e3, o3),
        sub(e0, o0),
        sub(e1, o1),
        plus_turn(e2, o2, -sign),
        add(e3, o3),
    ]


def halves(x):
    high = x.astype(BF16)
    return high, (x - high.astype(F32)).astype(BF16)


def mm(left, right):
    return jnp.dot(left, right, preferred_element_type=F32)


def split_table(table):
    table = np.asarray(table, np.float32)
    high = table.astype(BF16)
    low = (table - high.astype(np.float32)).astype(BF16)
    return jnp.asarray(np.stack([high, low]))


def dft_real(length):
    idx = np.arange(length)
    angles = 2.0 * np.pi / length * (idx[:, None] * idx[None, :] % length)
    cos, sin = np.cos(angles), np.sin(angles)
    return np.block([[cos, -sin], [sin, cos]])


def three(high, low):
    return jnp.concatenate([high, low, high], axis=-1)


def prepare(axis, n1, wave_ref, tw1_ref, phase_ref, tw2_ref, filt_ref, flat, turned):
    me = lax.axis_index(axis)
    count = phase_ref.shape[1]
    ways = LANES // n1
    for part in range(2):
        for m in range(n1):
            flat[m : m + 1, :] = wave_ref[part : part + 1, m * LANES : (m + 1) * LANES]
        rows = flat[:n1, :]
        for h in range(ways):
            moved = pltpu.roll(rows, LANES - h * n1, 1) if h else rows
            flat[pl.ds(h, n1, stride=ways), :] = moved
        turned[...] = flat[...].T
        for k in range(n1):
            at = k % RADIX * (n1 // RADIX) + k // RADIX
            filt_ref[part, at : at + 1, :] = turned[k : k + 1, :]
    for part in range(2):
        for k in range(n1):
            at = k * me % count
            tw2_ref[part, k : k + 1, :] = phase_ref[part, pl.ds(at, 1), :]
    turn_re, turn_im = tw2_ref[0], tw2_ref[1]
    cos, sin = tw1_ref[0], tw1_ref[1]
    tw2_ref[0] = cos * turn_re - sin * turn_im
    tw2_ref[1] = sin * turn_re + cos * turn_im


def compress_body(axis, pieces, hops, count, x_ref, taper_ref, wave_ref, tab_ref, tw1_ref, phase_ref, *rest):
    me = lax.axis_index(axis)
    outs, used = [], 0
    for hop in hops:
        if hop:
            outs.append(rest[used : used + count])
            used += count
        else:
            outs.append([rest[used].at[(me + k) % count] for k in range(count)])
            used += 1
    stage, grid, back, tw2_ref, filt_ref, flat, turned = rest[used:]
    own = x_ref.shape[3]
    n1 = x_ref.shape[4] // LANES
    depth = n1 // RADIX
    tiles = n1 // count
    step = pl.program_id(0)

    @pl.when(step == 0)
    def _():
        prepare(axis, n1, wave_ref, tw1_ref, phase_ref, tw2_ref, filt_ref, flat, turned)

    def rows(ref, i, k):
        return jnp.broadcast_to(ref[i, k : k + 1, :], (SUB, LANES))

    place = {}
    for p, piece in enumerate(pieces):
        for at, tile in enumerate(piece):
            place[tile] = (p, at)
    row = lax.broadcasted_iota(jnp.int32, (SUB, LANES), 0)
    first = (me * pl.num_programs(0) + step) * own
    root = 1.0 / math.sqrt(taper_ref.shape[0])
    groups = [slice(g * SUB, (g + 1) * SUB) for g in range(own // SUB)]
    for g, at in enumerate(groups):
        taper = jnp.full((SUB, LANES), taper_ref[first + g * SUB])
        for r in range(1, SUB):
            taper = jnp.where(row == r, taper_ref[first + g * SUB + r], taper)
        taper = taper * root
        for b in range(depth):
            x = []
            for a in range(RADIX):
                cols = slice((depth * a + b) * LANES, (depth * a + b + 1) * LANES)
                x.append((x_ref[0, 0, 0, at, cols] * taper, x_ref[0, 1, 0, at, cols] * taper))
            for c, y in enumerate(dft8(x, -1)):
                y = times(y, -2.0 * math.pi * b * c / n1)
                stage[g, 0, c * depth + b] = y[0]
                stage[g, 1, c * depth + b] = y[1]
    table = jnp.concatenate([tab_ref[0], tab_ref[0], tab_ref[1]], axis=0)
    span = RADIX // CHUNKS
    wide = span * depth

    def spread(n):
        for g, at in enumerate(groups):
            for c in range(n * span, (n + 1) * span):
                x = [(stage[g, 0, c * depth + b], stage[g, 1, c * depth + b]) for b in range(depth)]
                for d, y in enumerate(dft8(x, -1)):
                    k = c + RADIX * d
                    cos, sin = rows(tw1_ref, 0, k), rows(tw1_ref, 1, k)
                    grid[n, (c - n * span) * depth + d, at, :LANES] = y[0] * cos + y[1] * sin
                    grid[n, (c - n * span) * depth + d, at, LANES:] = y[1] * cos - y[0] * sin

    def transform(values):
        return mm(three(*halves(values.reshape(wide * own, 2 * LANES))), table)

    def filtered(n, spec):
        spec = spec.reshape(wide, own, 2 * LANES)
        s_re, s_im = spec[:, :, :LANES], spec[:, :, LANES:]
        here = slice(n * wide, (n + 1) * wide)
        f_re, f_im = filt_ref[0, here][:, None, :], filt_ref[1, here][:, None, :]
        z_re = s_re * f_re + s_im * f_im
        z_im = s_re * f_im - s_im * f_re
        return jnp.concatenate([z_re, z_im], axis=-1)

    def gather(n):
        for g, at in enumerate(groups):
            for c in range(n * span, (n + 1) * span):
                x = []
                for d in range(depth):
                    k = c + RADIX * d
                    cos, sin = rows(tw2_ref, 0, k), rows(tw2_ref, 1, k)
                    v = back[n, (c - n * span) * depth + d, at, :]
                    v_re, v_im = v[:, :LANES], v[:, LANES:]
                    x.append((v_re * cos + v_im * sin, v_re * sin - v_im * cos))
                for b, y in enumerate(dft8(x, 1)):
                    y = times(y, 2.0 * math.pi * b * c / n1)
                    stage[g, 0, b * RADIX + c] = y[0]
                    stage[g, 1, b * RADIX + c] = y[1]

    for n in range(CHUNKS):
        spread(n)
        spec = transform(grid[n])
        back[n] = transform(filtered(n, spec)).reshape(wide, own, 2 * LANES)
    for n in range(CHUNKS):
        gather(n)
    for g, at in enumerate(groups):
        for b in range(depth):
            x = [(stage[g, 0, b * RADIX + c], stage[g, 1, b * RADIX + c]) for c in range(RADIX)]
            for a, y in enumerate(dft8(x, 1)):
                k, j = divmod(depth * a + b, tiles)
                p, to = place[j]
                out = outs[p][k]
                out[0, at, to * LANES : (to + 1) * LANES] = y[0]
                out[1, at, to * LANES : (to + 1) * LANES] = y[1]


def whole(shape):
    return pl.BlockSpec(shape, lambda i: (0,) * len(shape))


def compress(axis, echoes, beam, pieces, hops, taper, wave, tab, tw1, phase):
    pulses, gates = echoes.shape[3:]
    count = phase.shape[1]
    n1 = gates // LANES
    size = math.gcd(pulses, SUB * GROUPS)
    shapes, specs = [], []
    for piece, hop in zip(pieces, hops):
        wide = len(piece) * LANES
        if hop:
            shapes += [jax.ShapeDtypeStruct((2, pulses, wide), F32)] * count
            specs += [pl.BlockSpec((2, size, wide), lambda i: (0, i, 0))] * count
        else:
            shapes.append(jax.ShapeDtypeStruct((count, 2, pulses, wide), F32))
            specs.append(pl.BlockSpec((count, 2, size, wide), lambda i: (0, 0, i, 0)))
    out = pl.pallas_call(
        partial(compress_body, axis, pieces, hops, count),
        grid=(pulses // size,),
        in_specs=[
            pl.BlockSpec((1, 2, 1, size, gates), lambda i: (0, 0, beam, i, 0)),
            pl.BlockSpec(memory_space=pltpu.SMEM),
            whole(wave.shape),
            whole(tab.shape),
            whole(tw1.shape),
            whole(phase.shape),
        ],
        out_specs=specs,
        out_shape=shapes,
        scratch_shapes=[
            pltpu.VMEM((size // SUB, 2, n1, SUB, LANES), F32),
            pltpu.VMEM((CHUNKS, n1 // CHUNKS, size, 2 * LANES), F32),
            pltpu.VMEM((CHUNKS, n1 // CHUNKS, size, 2 * LANES), F32),
            pltpu.VMEM((2, n1, LANES), F32),
            pltpu.VMEM((2, n1, LANES), F32),
            pltpu.VMEM((LANES, LANES), F32),
            pltpu.VMEM((LANES, LANES), F32),
        ],
        cost_estimate=pl.CostEstimate(
            flops=pulses * gates * 6000, transcendentals=0, bytes_accessed=pulses * gates * 16
        ),
        name="compress",
    )(echoes, taper, wave, tab, tw1, phase)
    blocks = []
    for hop in hops:
        blocks.append(out[:count] if hop else out[0])
        out = out[count if hop else 1 :]
    return blocks


def doppler_core(ins, pulses, tab_ref, tw_ref, high_buf, low_buf, emit):
    if len(ins) == 1:
        ins = [ins[0].at[k] for k in range(ins[0].shape[0])]
    own = ins[0].shape[1]
    tiles = ins[0].shape[2] // LANES
    quarter = pulses // 4

    def load(part, start, lanes):
        slot, row = divmod(start, own)
        return ins[slot][part, row : row + SUB, lanes]

    for r in range(0, quarter, 2 * SUB):
        for j in range(tiles):
            lanes = slice(j * LANES, (j + 1) * LANES)
            x = []
            for h in range(4):
                x.append(
                    tuple(
                        jnp.concatenate(
                            [load(part, h * quarter + r + s, lanes) for s in (0, SUB)], axis=0
                        )
                        for part in range(2)
                    )
                )
            for k, y in enumerate(dft4(*x, -1)):
                if k:
                    cos = tw_ref[k - 1, 0, r : r + 2 * SUB, :]
                    sin = tw_ref[k - 1, 1, r : r + 2 * SUB, :]
                    y = (y[0] * cos + y[1] * sin, y[1] * cos - y[0] * sin)
                for part in range(2):
                    high, low = halves(y[part])
                    at = part * quarter + r
                    high_buf[k, at : at + 2 * SUB, lanes] = high
                    low_buf[k, at : at + 2 * SUB, lanes] = low
    table = jnp.concatenate([tab_ref[0], tab_ref[0], tab_ref[1]], axis=1)
    for k in range(4):
        high, low = high_buf[k], low_buf[k]
        out = mm(table, jnp.concatenate([high, low, high], axis=0))
        power = out[:quarter] * out[:quarter] + out[quarter:] * out[quarter:]
        for j in range(tiles):
            emit(j, pl.ds(k, quarter, stride=4), power[:, j * LANES : (j + 1) * LANES])


def doppler_body(count, pulses, ends, tab_ref, tw_ref, *rest):
    ins = rest[:count]
    power_ref, left_ref, right_ref, high_buf, low_buf = rest[count:]

    def emit(j, rows, value):
        power_ref[j, rows, :] = value

    doppler_core(ins, pulses, tab_ref, tw_ref, high_buf, low_buf, emit)
    left_ref[...] = power_ref[ends[0]].T[:EDGE]
    right_ref[...] = power_ref[ends[1]].T[LANES - EDGE :]


def doppler(blocks, tab, tw, pulses, ends):
    count = len(blocks)
    width = blocks[0].shape[-1]
    tiles = width // LANES
    half = pulses // 2
    return pl.pallas_call(
        partial(doppler_body, count, pulses, ends),
        out_shape=[
            jax.ShapeDtypeStruct((tiles, pulses, LANES), F32),
            jax.ShapeDtypeStruct((EDGE, pulses), F32),
            jax.ShapeDtypeStruct((EDGE, pulses), F32),
        ],
        scratch_shapes=[pltpu.VMEM((4, half, width), BF16), pltpu.VMEM((4, half, width), BF16)],
        cost_estimate=pl.CostEstimate(
            flops=pulses * width * 6000, transcendentals=0, bytes_accessed=pulses * width * 12
        ),
        name="doppler",
    )(tab, tw, *blocks)


def cfar_core(beam, tiles, guard_ref, train_ref, floor_ref, left, right, tile, high_buf, low_buf, emit):
    pulses = high_buf.shape[0]
    group = 2 if tiles % 2 == 0 else 1
    guard, train = guard_ref[beam], train_ref[beam]
    width = group * LANES
    rows = width + 2 * LANES
    shape = (rows, width)
    away = jnp.abs(
        lax.broadcasted_iota(jnp.int32, shape, 0)
        - LANES
        - lax.broadcasted_iota(jnp.int32, shape, 1)
    )
    band = jnp.where((away > guard) & (away <= guard + train), 1.0, 0.0).astype(BF16)
    blank = jnp.zeros((LANES - EDGE, pulses), F32)
    floor = jnp.full((1, LANES), floor_ref[beam])
    scale = 0.5 / jnp.full((1, LANES), train.astype(F32))
    for t in range(tiles + 2):
        if t == 0:
            values = jnp.concatenate([blank, left], axis=0).T
        elif t == tiles + 1:
            values = jnp.concatenate([right, blank], axis=0).T
        else:
            values = tile(t - 1)
        high, low = halves(values)
        high_buf[:, t * LANES : (t + 1) * LANES] = high
        low_buf[:, t * LANES : (t + 1) * LANES] = low
    twice = jnp.concatenate([band, band], axis=0)
    for t in range(0, tiles, group):
        cols = slice(t * LANES, t * LANES + rows)
        window = mm(jnp.concatenate([high_buf[:, cols], low_buf[:, cols]], axis=1), twice)
        for g in range(group):
            noise = floor + window[:, g * LANES : (g + 1) * LANES] * scale
            emit(t + g, tile(t + g) / noise)


def finish_body(beam, count, known, fresh, pulses, *refs):
    guard_ref, train_ref, floor_ref, left_ref, right_ref = refs[:5]
    refs = refs[5:]
    tiles = len(known) + len(fresh)
    old = new = None
    if known:
        old, refs = refs[0], refs[1:]
    if fresh:
        tab_ref, tw_ref = refs[:2]
        ins = refs[2 : 2 + count]
        refs = refs[2 + count :]
    bufs = refs[len(refs) - (5 if fresh else 2) :]
    out_ref = refs[len(refs) - len(bufs) - 1]
    if fresh:
        new = bufs[4]

        def keep(j, rows, value):
            new[j, rows, :] = value

        doppler_core(ins, pulses, tab_ref, tw_ref, bufs[2], bufs[3], keep)

    def tile(t):
        return old[known.index(t)] if t in known else new[fresh.index(t)]

    def emit(t, value):
        out_ref[0, 0, :, t * LANES : (t + 1) * LANES] = value

    cfar_core(
        beam, tiles, guard_ref, train_ref, floor_ref, left_ref[...], right_ref[...], tile, bufs[0], bufs[1], emit
    )


def finish(beam, beams, scalars, left, right, known, power, fresh, blocks, tables, prior):
    pulses = left.shape[1]
    tiles = len(known) + len(fresh)
    width = tiles * LANES
    smem = pl.BlockSpec(memory_space=pltpu.SMEM)
    args = list(scalars) + [left, right]
    if known:
        args.append(power)
    if fresh:
        args += list(tables) + list(blocks)
    specs = [smem] * len(scalars) + [whole(a.shape) for a in args[len(scalars) :]]
    alias = {}
    if prior is not None:
        args.append(prior)
        specs.append(pl.BlockSpec(memory_space=pl.ANY))
        alias = {len(args) - 1: 0}
    scratch = [pltpu.VMEM((pulses, width + 2 * LANES), BF16)] * 2
    if fresh:
        scratch += [pltpu.VMEM((4, pulses // 2, len(fresh) * LANES), BF16)] * 2
        scratch += [pltpu.VMEM((len(fresh), pulses, LANES), F32)]
    return pl.pallas_call(
        partial(finish_body, beam, len(blocks), known, fresh, pulses),
        grid=(1,),
        in_specs=specs,
        out_specs=pl.BlockSpec((1, 1, pulses, width), lambda i: (0, beam, 0, 0)),
        out_shape=jax.ShapeDtypeStruct((1, beams, pulses, width), F32),
        scratch_shapes=scratch,
        input_output_aliases=alias,
        cost_estimate=pl.CostEstimate(
            flops=pulses * width * 4000, transcendentals=0, bytes_accessed=pulses * width * 8
        ),
        name="finish",
    )(*args)


def exchange(blocks, axis):
    if not isinstance(blocks, (tuple, list)):
        return [lax.all_to_all(blocks, axis, 0, 0, tiled=True)]
    count = len(blocks)
    got = [blocks[0]] + [None] * (count - 1)
    for k in range(1, count):
        ring = [(i, (i + k) % count) for i in range(count)]
        got[(count - k) % count] = lax.ppermute(blocks[k], axis, ring)
    return got


def modes(count):
    return MODES if count <= 16 else (False,) * len(MODES)


def halo(axis, first, last):
    count = lax.axis_size(axis)
    left = lax.ppermute(last, axis, [(i, i + 1) for i in range(count - 1)])
    right = lax.ppermute(first, axis, [(i + 1, i) for i in range(count - 1)])
    return left, right


def shards_inner(axis, echoes, waveform, doppler_taper, cfar_guard, cfar_train, noise_floor):
    count = lax.axis_size(axis)
    beams, own, gates = echoes.shape[2:]
    pulses = own * count
    n1 = gates // LANES
    tiles = n1 // count

    tab = split_table(dft_real(LANES))
    angles = 2.0 * np.pi / gates * (np.arange(n1)[:, None] * np.arange(LANES)[None, :])
    tw1 = jnp.asarray(np.stack([np.cos(angles), np.sin(angles)]), F32)
    angles = 2.0 * np.pi / count * np.arange(count)
    phase = np.stack([np.cos(angles), np.sin(angles)])[..., None] / gates
    phase = jnp.asarray(np.broadcast_to(phase, phase.shape[:2] + (LANES,)), F32)
    quarter = pulses // 4
    dop_tab = split_table(dft_real(quarter).T)
    turns = 2.0 * np.pi / pulses * (np.arange(1, 4)[:, None] * np.arange(quarter)[None, :])
    turns = np.stack([np.cos(turns), np.sin(turns)], axis=1)[..., None]
    dop_tw = jnp.asarray(np.broadcast_to(turns, turns.shape[:3] + (LANES,)), F32)
    tables = (dop_tab, dop_tw)
    scalars = (cfar_guard, cfar_train, noise_floor)

    every = tuple(range(tiles))
    middle = every[tiles // 2 : tiles // 2 + 1] if tiles > 2 else ()
    outer = tuple(t for t in every if t not in middle)
    built = []
    for beam in range(beams):
        split = middle and beam == beams - 1
        pieces = (outer, middle) if split else (every,)
        hops = modes(count)[len(built) : len(built) + len(pieces)]
        blocks = compress(
            axis, echoes, beam, pieces, hops, doppler_taper, waveform, tab, tw1, phase
        )
        built += [(beam, piece, block) for piece, block in zip(pieces, blocks)]
    sent = []
    for beam, piece, block in built:
        sent.append((beam, piece, exchange(block, axis)))
    known = []
    late = None
    gate = [block[0] if isinstance(block, list) else block for _, _, block in built]
    for beam, piece, blocks in sent:
        if 0 not in piece:
            late = (piece, blocks)
            continue
        blocks, gate = lax.optimization_barrier((blocks, gate))
        power, first, last = doppler(blocks, *tables, pulses, (0, len(piece) - 1))
        gate = (gate, power)
        left, right = halo(axis, first, last)
        known.append((beam, left, right, piece, power))
    result = None
    for beam, left, right, piece, power in known:
        args = (beam, beams, scalars, left, right, piece, power)
        if len(piece) < tiles:
            fresh, blocks = late
            blocks, result = lax.optimization_barrier((blocks, result))
            result = finish(*args, fresh, blocks, tables, result)
        else:
            result = finish(*args, (), (), tables, result)
    return result


def shards(axis, *args):
    return shards_inner(axis, *args)


def solution(mesh):
    in_specs = (
        P(None, None, "groups", "shard", None),
        P(),
        P(),
        P("groups"),
        P("groups"),
        P("groups"),
    )
    out_specs = P(None, "groups", None, "shard")
    return jax.shard_map(
        partial(shards, "shard"), mesh=mesh, in_specs=in_specs, out_specs=out_specs, check_vma=False
    )
```
